32 devices in a mesh: ta: 4 (over z), gz: 4 (over x, core), xy: 2 (over y).
Axes of the slice: x: 2, y: 2, z: 4, core: 2. Of those that a mesh axis runs over, the one named last changes fastest.
Arguments:
- links: float32 [4, 2, 3, 3, 4, 8, 512], P(None, None, None, None, 'ta', 'xy', 'gz'), may hold values from -0.72 to 1.72
- guess: float32 [12, 2, 4, 3, 4, 8, 512], P(None, None, None, None, 'ta', 'xy', 'gz'), may hold values from -1.5 to 1.5
- source_sites: int32 [4, 2, 4, 4], P('ta', 'xy', 'gz'), may hold values from 0 to 31, as said below
Outputs:
- solution: float32 [12, 2, 4, 3, 4, 8, 512], P(None, None, None, None, 'ta', 'xy', 'gz')
- residual: float32 [12, 2, 4, 3, 4, 8, 512], P(None, None, None, None, 'ta', 'xy', 'gz')
The draws below stay inside these ranges and needn't reach their ends.
Inputs may be any that keep to these rules, and one draw needn't show every extreme that they name: `source_sites`: each entry is an offset inside its block: time below 1, y below 4, z below 4, x below 32.
All inputs are finite; a program needn't handle non-finite values.
Results may differ from the reference program's by a relative error of at most 0.00012.
Values sent between devices are 32-bit elements; how exact they have to be, the bound alone decides.
A program may use at most 128 MiB of HBM per device.

```python
import math
import jax
import jax.numpy as jnp
import numpy as np
from jax import lax

LT = 1
LY = 4
LZ = 4
LX = 32
NSMEAR = 8
NT = 4
NY = 8
NZ = 16


def draw_links(key, part):
    full_shape = (4, 2, 3, 3, NT, NY, NZ * LX)
    noise = 0.18 * jnp.clip(jax.random.normal(key, full_shape), -4.0, 4.0)
    identity = jnp.eye(3, dtype=jnp.float32)
    unit = jnp.stack([identity, jnp.zeros_like(identity)], axis=0)
    return (unit[None, :, :, :, None, None, None] + noise).astype(jnp.float32)


def draw_guess(key, part):
    main_key, slice_key = jax.random.split(key)
    full_shape = (12, 2, 4, 3, NT, NY, NZ * LX)
    rising = 10.0 ** (jnp.arange(NT, dtype=jnp.float32) / NT)
    slices = jax.random.uniform(slice_key, (NZ,), minval=0.0, maxval=math.log(3.0))
    slice_scale = jnp.repeat(jnp.exp(slices), LX)
    noise = jnp.clip(jax.random.normal(main_key, full_shape), -5.0, 5.0)
    return (0.01 * noise * rising[:, None, None] * slice_scale).astype(jnp.float32)


def draw_source_sites(key, part):
    blocks = (NT // LT, NY // LY, NZ // LZ)
    subkeys = jax.random.split(key, 4)
    limits = (LT, LY, LZ, LX)
    columns = [jax.random.randint(subkeys[position], blocks, 0, limits[position]) for position in range(4)]
    return jnp.stack(columns, axis=-1).astype(jnp.int32)


def setup_inputs(seed: int = 0) -> dict:
    arg_keys = jax.random.split(jax.random.key(seed), 4)
    links = draw_links(jax.random.fold_in(arg_keys[3], 71), 0)
    guess = draw_guess(jax.random.fold_in(arg_keys[3], 71), 0)
    source_sites = draw_source_sites(jax.random.fold_in(arg_keys[3], 71), 0)
    return dict(links=links, guess=guess, source_sites=source_sites)


HIGHEST = lax.Precision.HIGHEST
hopping = 0.12
smear_weight = 0.25
smear_norm = 2.0


def pauli_blocks():
    sigma_one = np.array([[0, 1], [1, 0]], dtype=complex)
    sigma_two = np.array([[0, -1j], [1j, 0]], dtype=complex)
    sigma_three = np.array([[1, 0], [0, -1]], dtype=complex)
    return [-1j * sigma_one, -1j * sigma_two, -1j * sigma_three, np.eye(2, dtype=complex)]


def real_form(matrix):
    upper = np.concatenate([matrix.real, -matrix.imag], axis=1)
    lower = np.concatenate([matrix.imag, matrix.real], axis=1)
    return np.concatenate([upper, lower], axis=0).astype(np.float32)


def full_table(direction, parity):
    block_matrix = pauli_blocks()[direction]
    project_rows = np.concatenate([np.eye(2), parity * block_matrix], axis=1)
    lift_rows = np.concatenate([np.eye(2), parity * block_matrix.conj().T], axis=0)
    return real_form(lift_rows @ project_rows)


def spin_apply(matrix, field):
    spin_table = jnp.asarray(matrix)
    copies = field.shape[0]
    flattened = field.reshape((copies, spin_table.shape[1]) + field.shape[3:])
    applied = jnp.einsum('ij,rjatyw->riatyw', spin_table, flattened, precision=HIGHEST)
    return applied.reshape((copies, 2, spin_table.shape[0] // 2) + field.shape[3:])


def colour_times(link, field, adjoint):
    form = 'batyw,...btyw->...atyw' if adjoint else 'abtyw,...btyw->...atyw'
    parity = -1.0 if adjoint else 1.0
    real_part = field[:, 0]
    imag_part = field[:, 1]
    out_real = jnp.einsum(form, link[0], real_part, precision=HIGHEST) - parity * jnp.einsum(form, link[1], imag_part, precision=HIGHEST)
    out_imag = jnp.einsum(form, link[0], imag_part, precision=HIGHEST) + parity * jnp.einsum(form, link[1], real_part, precision=HIGHEST)
    return jnp.stack([out_real, out_imag], axis=1)


def roll_x(field, amount):
    shaped = field.reshape(field.shape[:-1] + (field.shape[-1] // LX, LX))
    return jnp.roll(shaped, amount, axis=-1).reshape(field.shape)


def shift_ahead(field, direction):
    if direction == 0:
        return roll_x(field, -1)
    if direction == 1:
        return jnp.roll(field, -1, axis=-2)
    if direction == 2:
        return jnp.roll(field, -LX, axis=-1)
    return jnp.roll(field, -1, axis=-3)


def shift_behind(field, direction):
    if direction == 0:
        return roll_x(field, 1)
    if direction == 1:
        return jnp.roll(field, 1, axis=-2)
    if direction == 2:
        return jnp.roll(field, LX, axis=-1)
    return jnp.roll(field, 1, axis=-3)


def point_sources(source_sites):
    time_ids = jnp.arange(NT, dtype=jnp.int32)
    row_ids = jnp.arange(NY, dtype=jnp.int32)
    slice_ids = jnp.arange(NZ, dtype=jnp.int32)
    column_ids = jnp.arange(LX, dtype=jnp.int32)
    offsets = source_sites[(time_ids // LT)[:, None, None], (row_ids // LY)[None, :, None], (slice_ids // LZ)[None, None, :]]
    site_hit = (offsets[..., 0] == (time_ids % LT)[:, None, None]) & (offsets[..., 1] == (row_ids % LY)[None, :, None]) & (offsets[..., 2] == (slice_ids % LZ)[None, None, :])
    site_hit = site_hit[..., None] & (offsets[..., 3:4] == column_ids)
    mask = jnp.where(site_hit, 1.0, 0.0).astype(jnp.float32).reshape(NT, NY, NZ * LX)
    identity = jnp.eye(3, dtype=jnp.float32)
    real_part = identity[:, :, None, None, None] * mask
    return jnp.stack([real_part, jnp.zeros_like(real_part)], axis=1)


def smear_step(colour_field, links):
    total = jnp.zeros_like(colour_field)
    for direction in range(3):
        link = links[direction]
        ahead_part = colour_times(link, shift_ahead(colour_field, direction), False)
        behind_part = shift_behind(colour_times(link, colour_field, True), direction)
        total = total + ahead_part + behind_part
    return (colour_field + smear_weight * total) / smear_norm


def spread(colour_field):
    identity = jnp.eye(4, dtype=jnp.float32)
    grown = identity[:, None, None, :, None, None, None, None] * colour_field[None, :, :, None, :, :, :, :]
    return grown.reshape((12, 2, 4, 3) + colour_field.shape[3:])


def wilson_single(field, links):
    time_ids = jnp.arange(NT, dtype=jnp.int32)
    ahead_parity = jnp.where(time_ids == NT - 1, -1.0, 1.0).astype(jnp.float32)[:, None, None]
    behind_parity = jnp.where(time_ids == 0, -1.0, 1.0).astype(jnp.float32)[:, None, None]
    total = jnp.zeros_like(field)
    for direction in range(4):
        link = links[direction]
        ahead_part = shift_ahead(field, direction)
        behind_part = shift_behind(colour_times(link, field, True), direction)
        if direction == 3:
            ahead_part = ahead_part * ahead_parity
            behind_part = behind_part * behind_parity
        ahead_part = colour_times(link, ahead_part, False)
        total = total + spin_apply(full_table(direction, -1.0), ahead_part) + spin_apply(full_table(direction, 1.0), behind_part)
    return field - hopping * total


def wilson(field, links):
    return lax.map(lambda single: wilson_single(single[None], links)[0], field)


def dagger(field, links):
    chirality = jnp.array([1.0, 1.0, -1.0, -1.0], dtype=jnp.float32)[None, None, :, None, None, None, None]
    return chirality * wilson(chirality * field, links)


def reference(links, guess, source_sites):
    colour_field = point_sources(source_sites)
    for iteration in range(NSMEAR):
        colour_field = smear_step(colour_field, links)
    right_side = spread(colour_field)
    defect = right_side - wilson(guess, links)
    search = dagger(defect, links)
    applied = wilson(search, links)
    summed_axes = (1, 2, 3, 4, 5, 6)
    norm_now = jnp.sum(search * search, axis=summed_axes)
    curvature = jnp.sum(applied * applied, axis=summed_axes)
    step_length = (norm_now / curvature)[:, None, None, None, None, None, None]
    solution = guess + step_length * search
    residual = search - step_length * dagger(applied, links)
    return solution, residual
```

```python
import functools

import jax
import jax.numpy as jnp
from jax import lax
from jax.experimental import pallas as pl
from jax.experimental.pallas import tpu as pltpu
from jax.sharding import PartitionSpec as P

LX = 32
NSMEAR = 8
HOP = 0.12
PAIRS = 6
MESH = pl.DeviceIdType.MESH
AXES = ("xy", "gz", "ta")

E_ROWS = (
    ((1, -1j), (0, -1j)),
    ((1, -1), (0, 1)),
    ((0, -1j), (1, 1j)),
    ((0, 1), (1, 1)),
)


def times(coef, z):
    re, im = z
    if coef == 1:
        return (1, re), (1, im)
    if coef == -1:
        return (-1, re), (-1, im)
    if coef == 1j:
        return (-1, im), (1, re)
    return (1, im), (-1, re)


def add_term(z, coef, other):
    out = []
    for base, (sign, term) in zip(z, times(coef, other)):
        out.append(base + term if sign > 0 else base - term)
    return tuple(out)


def project(f, mu, parity):
    half = []
    for row in range(2):
        column, coef = E_ROWS[mu][row]
        half.append([add_term(f[row][a], parity * coef, f[2 + column][a]) for a in range(3)])
    return half


def lift_add(total, h, mu, parity):
    for row in range(2):
        column, coef = E_ROWS[mu][row]
        for a in range(3):
            total[row][a] = add_term(total[row][a], 1, h[row][a])
            low = parity * complex(coef).conjugate()
            total[2 + column][a] = add_term(total[2 + column][a], low, h[row][a])


def link_times(link, mu, vectors, adjoint):
    def entry(a, b):
        if adjoint:
            a, b = b, a
        base = mu * 18 + a * 3 + b
        return link[base], link[base + 9]

    out = [[None] * 3 for _ in vectors]
    for a in range(3):
        totals = [None] * len(vectors)
        for b in range(3):
            ur, ui = entry(a, b)
            for k, vec in enumerate(vectors):
                re, im = vec[b]
                if adjoint:
                    tr, ti = ur * re + ui * im, ur * im - ui * re
                else:
                    tr, ti = ur * re - ui * im, ur * im + ui * re
                old = totals[k]
                totals[k] = (tr, ti) if old is None else (old[0] + tr, old[1] + ti)
        for k in range(len(vectors)):
            out[k][a] = totals[k]
    return out


def flat(vectors):
    return [vec[a][part] for part in range(2) for vec in vectors for a in range(3)]


def unflat(items, count):
    return [
        [(items[k * 3 + a], items[3 * count + k * 3 + a]) for a in range(3)] for k in range(count)
    ]


class Shifts:
    def __init__(self):
        row = lax.broadcasted_iota(jnp.int32, (8, 128), 0)
        lane = lax.broadcasted_iota(jnp.int32, (8, 128), 1)
        self.low = row < 4
        self.lane = lane
        self.place = ([row % 4 == k for k in range(4)], [lane // LX == k for k in range(4)])
        self.x_first = lane % LX == 0
        self.x_last = lane % LX == LX - 1
        self.unit = ((0, 1, 8), (1, LX, 128))

    def roll(self, v, kind, steps):
        axis, unit, size = self.unit[kind]
        amount = (steps * unit) % size
        return v if amount == 0 else pltpu.roll(v, amount, axis)

    def pack(self, items, kind, ahead):
        packed = []
        for g in range(0, len(items), 4):
            out = None
            for k in range(4):
                v = self.roll(items[g + k], kind, k if ahead else k - 3)
                out = v if out is None else jnp.where(self.place[kind][k], v, out)
            packed.append(out)
        return packed

    def shift(self, items, packed, kind, ahead):
        outs = []
        for i, v in enumerate(items):
            got = packed[i // 4]
            k = i % 4
            if ahead:
                moved = self.roll(v, kind, -1)
                outs.append(jnp.where(self.place[kind][3], self.roll(got, kind, 3 - k), moved))
            else:
                moved = self.roll(v, kind, 1)
                outs.append(jnp.where(self.place[kind][0], self.roll(got, kind, -k), moved))
        return outs

    def along_x(self, items, ahead):
        outs = []
        for v in items:
            if ahead:
                a, b = pltpu.roll(v, 127, 1), pltpu.roll(v, LX - 1, 1)
                outs.append(jnp.where(self.x_last, b, a))
            else:
                a, b = pltpu.roll(v, 1, 1), pltpu.roll(v, 129 - LX, 1)
                outs.append(jnp.where(self.x_first, b, a))
        return outs


def kernel(
    sizes, sites_ref, links_ref, guess_ref, sol_ref, res_ref,
    link, guess, field_a, field_b, search, acc, right, carried,
    edge_out, edge_in, time_out, time_in, sm_out, sm_in, smt_out, smt_in,
    red_out, red_in, sums,
    edge_sem, time_sem, w_send, sm_sem, smt_sem, s_send, red_sem, r_send,
):
    n_of = dict(zip(AXES, sizes))
    me = {axis: lax.axis_index(axis) for axis in AXES}

    def peer(axis, step):
        return {axis: lax.rem(me[axis] + step + n_of[axis], n_of[axis])}

    barrier = pltpu.get_barrier_semaphore()
    for axis in AXES:
        for k in range(1, n_of[axis]):
            pl.semaphore_signal(barrier, inc=1, device_id=peer(axis, k), device_id_type=MESH)

    sh = Shifts()

    sign = jnp.where(me["ta"] == n_of["ta"] - 1, -1.0, 1.0).astype(jnp.float32)
    for i in range(72):
        v = links_ref[i]
        if i >= 54:
            v = v * sign
        link[i, 0:4, :] = v
        link[i, 4:8, :] = v

    def rhs_of(p):
        first = jnp.where(p < 4, 3 * p, 6 * p - 22)
        second = jnp.where(p < 4, 3 * p + 1, 6 * p - 19)
        return first, second

    def load_guess(p, _):
        first, second = rhs_of(p)
        for i in range(24):
            guess[p, i, 0:4, :] = guess_ref[first, i]
            guess[p, i, 4:8, :] = guess_ref[second, i]
        return _

    lax.fori_loop(0, PAIRS, load_guess, 0)
    pl.semaphore_wait(barrier, sum(n - 1 for n in sizes))

    def edge_copy(w, d, p):
        axis, step = (("xy", -1), ("xy", 1), ("gz", -1), ("gz", 1))[d]
        return pltpu.make_async_remote_copy(
            src_ref=edge_out.at[w, d, p], dst_ref=edge_in.at[w, d, p],
            send_sem=w_send.at[w, d, p], recv_sem=edge_sem.at[w, d, p],
            device_id=peer(axis, step), device_id_type=MESH,
        )

    def time_copy(w, d, p):
        return pltpu.make_async_remote_copy(
            src_ref=time_out.at[w, d, p], dst_ref=time_in.at[w, d, p],
            send_sem=w_send.at[w, 4 + d, p], recv_sem=time_sem.at[w, d, p],
            device_id=peer("ta", (-1, 1)[d]), device_id_type=MESH,
        )

    def load_field(ref, p):
        return unflat([ref[p, i] for i in range(24)], 4)

    def send_body(f, w, p, par):
        for i, v in enumerate(flat(project(f, 3, -par))):
            time_out[w, 0, p, i] = v
        time_copy(w, 0, p).start()
        for i, v in enumerate(flat(link_times(link, 3, project(f, 3, par), True))):
            time_out[w, 1, p, i] = v
        time_copy(w, 1, p).start()
        for kind, mu in ((0, 1), (1, 2)):
            for i, v in enumerate(sh.pack(flat(project(f, mu, -par)), kind, True)):
                edge_out[w, 2 * kind, p, i] = v
            edge_copy(w, 2 * kind, p).start()
            behind = flat(link_times(link, mu, project(f, mu, par), True))
            for i, v in enumerate(behind):
                carried[kind, p, i] = v
            for i, v in enumerate(sh.pack(behind, kind, False)):
                edge_out[w, 2 * kind + 1, p, i] = v
            edge_copy(w, 2 * kind + 1, p).start()

    def interior(src, par):
        def body(p, _):
            f = load_field(src, p)
            zero = jnp.zeros((8, 128), jnp.float32)
            total = [[(zero, zero)] * 3 for _ in range(4)]
            ahead = unflat(sh.along_x(flat(project(f, 0, -par)), True), 2)
            lift_add(total, link_times(link, 0, ahead, False), 0, -par)
            behind = flat(link_times(link, 0, project(f, 0, par), True))
            lift_add(total, unflat(sh.along_x(behind, False), 2), 0, par)
            for i, v in enumerate(flat(total)):
                acc[p, i] = v
            return _
        lax.fori_loop(0, PAIRS, body, 0)

    def receive_body(src, w, p, par):
        f = load_field(src, p)
        total = load_field(acc, p)
        for kind, mu in ((0, 1), (1, 2)):
            edge_copy(w, 2 * kind, p).wait_recv()
            got = [edge_in[w, 2 * kind, p, i] for i in range(3)]
            ahead = unflat(sh.shift(flat(project(f, mu, -par)), got, kind, True), 2)
            lift_add(total, link_times(link, mu, ahead, False), mu, -par)
            edge_copy(w, 2 * kind + 1, p).wait_recv()
            got = [edge_in[w, 2 * kind + 1, p, i] for i in range(3)]
            local = [carried[kind, p, i] for i in range(12)]
            lift_add(total, unflat(sh.shift(local, got, kind, False), 2), mu, par)
        time_copy(w, 0, p).wait_recv()
        ahead = unflat([time_in[w, 0, p, i] for i in range(12)], 2)
        lift_add(total, link_times(link, 3, ahead, False), 3, -par)
        time_copy(w, 1, p).wait_recv()
        lift_add(total, unflat([time_in[w, 1, p, i] for i in range(12)], 2), 3, par)
        return [a - HOP * b for a, b in zip(flat(f), flat(total))]

    def sm_copy(step, d):
        axis, hop = (("xy", -1), ("xy", 1), ("gz", -1), ("gz", 1))[d]
        return pltpu.make_async_remote_copy(
            src_ref=sm_out.at[step, d], dst_ref=sm_in.at[step, d],
            send_sem=s_send.at[step, d], recv_sem=sm_sem.at[step, d],
            device_id=peer(axis, hop), device_id_type=MESH,
        )

    def smt_copy(d):
        return pltpu.make_async_remote_copy(
            src_ref=smt_out.at[d], dst_ref=smt_in.at[d],
            send_sem=s_send.at[NSMEAR + 1, d], recv_sem=smt_sem.at[d],
            device_id=peer("ta", (-1, 1)[d]), device_id_type=MESH,
        )

    def colour_hops(items, step):
        vectors = unflat(items, 2)
        behinds = []
        for kind, mu in ((0, 1), (1, 2)):
            for i, v in enumerate(sh.pack(items, kind, True)):
                sm_out[step, 2 * kind, i] = v
            sm_copy(step, 2 * kind).start()
            behind = flat(link_times(link, mu, vectors, True))
            behinds.append(behind)
            for i, v in enumerate(sh.pack(behind, kind, False)):
                sm_out[step, 2 * kind + 1, i] = v
            sm_copy(step, 2 * kind + 1).start()
        aheads_out = [flat(link_times(link, 0, unflat(sh.along_x(items, True), 2), False))]
        behinds_out = [sh.along_x(flat(link_times(link, 0, vectors, True)), False)]
        for kind, mu in ((0, 1), (1, 2)):
            sm_copy(step, 2 * kind).wait_recv()
            got = [sm_in[step, 2 * kind, i] for i in range(3)]
            ahead = unflat(sh.shift(items, got, kind, True), 2)
            aheads_out.append(flat(link_times(link, mu, ahead, False)))
            sm_copy(step, 2 * kind + 1).wait_recv()
            got = [sm_in[step, 2 * kind + 1, i] for i in range(3)]
            behinds_out.append(sh.shift(behinds[kind], got, kind, False))
        return aheads_out, behinds_out

    def smear_step(step, items):
        aheads, behinds = colour_hops(list(items), step)
        out = []
        for i, v in enumerate(items):
            total = None
            for part in aheads + behinds:
                total = part[i] if total is None else total + part[i]
            out.append((v + 0.25 * total) * 0.5)
        return tuple(out)

    def start_right(items):
        for i, v in enumerate(items):
            smt_out[0, i] = v
        smt_copy(0).start()
        for i, v in enumerate(flat(link_times(link, 3, unflat(items, 2), True))):
            smt_out[1, i] = v
        smt_copy(1).start()

    def finish_right(items):
        aheads, behinds = colour_hops(items, NSMEAR)
        smt_copy(0).wait_recv()
        got = unflat([smt_in[0, i] for i in range(12)], 2)
        aheads.append(flat(link_times(link, 3, got, False)))
        smt_copy(1).wait_recv()
        behinds.append([smt_in[1, i] for i in range(12)])
        diag = []
        for i, v in enumerate(items):
            total = None
            for part in aheads + behinds:
                total = part[i] if total is None else total + part[i]
            diag.append(v - HOP * total)
        diag = unflat(diag, 2)
        gs = [
            unflat([-HOP * (a - b) for a, b in zip(aheads[mu], behinds[mu])], 2)
            for mu in range(4)
        ]
        zero = jnp.zeros((8, 128), jnp.float32)

        def block(s2, s, q, a):
            if s2 == s:
                return diag[q][a]
            if s2 // 2 == s // 2:
                return (zero, zero)
            out = (zero, zero)
            for mu in range(4):
                for row in range(2):
                    column, coef = E_ROWS[mu][row]
                    if s2 < 2 and row == s2 and column == s - 2:
                        out = add_term(out, coef, gs[mu][q][a])
                    if s2 >= 2 and column == s2 - 2 and row == s:
                        out = add_term(out, complex(coef).conjugate(), gs[mu][q][a])
            return out

        for s2 in range(4):
            for a in range(3):
                column = [block(s2, s, 0, a) for s in range(4)]
                lone = [block(s2, s, 1, a) for s in range(4)]
                for part in range(2):
                    i = part * 12 + s2 * 3 + a
                    for s in range(4):
                        right[s, i] = column[s][part]
                    right[4, i] = jnp.where(sh.low, lone[0][part], lone[1][part])
                    right[5, i] = jnp.where(sh.low, lone[2][part], lone[3][part])

    def first_send(p, _):
        send_body(load_field(guess, p), 0, p, 1)
        return _

    row = lax.broadcasted_iota(jnp.int32, (8, 128), 0)
    hit = (row % 4 == sites_ref[1]) & (sh.lane == sites_ref[2] * LX + sites_ref[3])
    hit = hit & (sites_ref[0] == 0)
    one = jnp.where(hit, 1.0, 0.0).astype(jnp.float32)
    zero = jnp.zeros((8, 128), jnp.float32)
    upper, lower = jnp.where(sh.low, one, 0.0), jnp.where(sh.low, 0.0, one)
    items = tuple(flat([
        [(upper, zero), (lower, zero), (zero, zero)],
        [(zero, zero), (zero, zero), (one, zero)],
    ]))

    lax.fori_loop(0, PAIRS, first_send, 0)
    items = lax.fori_loop(0, NSMEAR // 2, smear_step, items)
    interior(guess, 1)

    def second(p, _):
        out = receive_body(guess, 0, p, 1)
        for i, v in enumerate(out):
            field_a[p, i] = v
        send_body(unflat(out, 4), 1, p, -1)
        return _

    lax.fori_loop(0, PAIRS, second, 0)
    items = lax.fori_loop(NSMEAR // 2, NSMEAR, smear_step, items)
    items = list(items)
    start_right(items)
    finish_right(items)
    interior(field_a, -1)

    def third(p, _):
        out = receive_body(field_a, 1, p, -1)
        out = [right[p, i] - v for i, v in enumerate(out)]
        total = None
        for i, v in enumerate(out):
            search[p, i] = v
            total = v * v if total is None else total + v * v
        sums[p] = total
        send_body(unflat(out, 4), 2, p, 1)
        return _

    lax.fori_loop(0, PAIRS, third, 0)
    interior(search, 1)

    def fourth(p, _):
        out = receive_body(search, 2, p, 1)
        total = None
        for i, v in enumerate(out):
            field_b[p, i] = v
            total = v * v if total is None else total + v * v
        sums[PAIRS + p] = total
        send_body(unflat(out, 4), 3, p, -1)
        return _

    lax.fori_loop(0, PAIRS, fourth, 0)

    mine = jnp.zeros((8, 128), jnp.float32)
    for k in range(2 * PAIRS):
        mine = jnp.where(sh.lane == k, jnp.sum(sums[k], axis=1, keepdims=True), mine)
    slot = 0
    done_interior = False
    for stage, axis in enumerate(AXES):
        red_out[stage] = mine
        copies = []
        for k in range(1, n_of[axis]):
            copy = pltpu.make_async_remote_copy(
                src_ref=red_out.at[stage], dst_ref=red_in.at[slot],
                send_sem=r_send.at[slot], recv_sem=red_sem.at[slot],
                device_id=peer(axis, k), device_id_type=MESH,
            )
            copy.start()
            copies.append((copy, slot))
            slot += 1
        if not done_interior:
            interior(field_b, -1)
            done_interior = True
        for copy, place in copies:
            copy.wait()
            mine = mine + red_in[place]
    top = jnp.sum(mine[0:4], axis=0, keepdims=True)
    bottom = jnp.sum(mine[4:8], axis=0, keepdims=True)
    both = jnp.where(sh.low, top, bottom)
    curvature = pltpu.roll(both, 128 - PAIRS, 1)
    steps = both / jnp.where(sh.lane < PAIRS, curvature, 1.0)

    def last(p, _):
        out = receive_body(field_b, 3, p, -1)
        length = jnp.sum(jnp.where(sh.lane == p, steps, 0.0), axis=1, keepdims=True)
        first, second_rhs = rhs_of(p)
        for i, v in enumerate(out):
            s = search[p, i]
            res = s - length * v
            sol = guess[p, i] + length * s
            res_ref[first, i] = res[0:4]
            res_ref[second_rhs, i] = res[4:8]
            sol_ref[first, i] = sol[0:4]
            sol_ref[second_rhs, i] = sol[4:8]
        return _

    lax.fori_loop(0, PAIRS, last, 0)

    def drain_w(p, _):
        for w in range(4):
            for d in range(4):
                edge_copy(w, d, p).wait_send()
            for d in range(2):
                time_copy(w, d, p).wait_send()
        return _

    lax.fori_loop(0, PAIRS, drain_w, 0)

    def drain_s(step, _):
        for d in range(4):
            sm_copy(step, d).wait_send()
        return _

    lax.fori_loop(0, NSMEAR + 1, drain_s, 0)
    for d in range(2):
        smt_copy(d).wait_send()


def on_device(sizes, links, guess, source_sites):
    rows, lanes = guess.shape[-2:]
    f32 = jnp.float32
    copies = sum(n - 1 for n in sizes)
    tile = (8, lanes)
    vm = lambda *shape: pltpu.VMEM(shape + tile, f32)
    dma = lambda *shape: pltpu.SemaphoreType.DMA(shape)
    out = jax.ShapeDtypeStruct((12, 24, rows, lanes), f32)
    sol, res = pl.pallas_call(
        functools.partial(kernel, sizes),
        out_shape=(out, out),
        in_specs=[
            pl.BlockSpec(memory_space=pltpu.SMEM),
            pl.BlockSpec(memory_space=pltpu.VMEM),
            pl.BlockSpec(memory_space=pltpu.VMEM),
        ],
        out_specs=(pl.BlockSpec(memory_space=pltpu.VMEM), pl.BlockSpec(memory_space=pltpu.VMEM)),
        scratch_shapes=[
            vm(72), vm(PAIRS, 24), vm(PAIRS, 24), vm(PAIRS, 24), vm(PAIRS, 24), vm(PAIRS, 24),
            vm(PAIRS, 24), vm(2, PAIRS, 12),
            vm(4, 4, PAIRS, 3), vm(4, 4, PAIRS, 3), vm(4, 2, PAIRS, 12), vm(4, 2, PAIRS, 12),
            vm(NSMEAR + 1, 4, 3), vm(NSMEAR + 1, 4, 3), vm(2, 12), vm(2, 12),
            vm(3), vm(copies), vm(2 * PAIRS),
            dma(4, 4, PAIRS), dma(4, 2, PAIRS), dma(4, 6, PAIRS),
            dma(NSMEAR + 1, 4), dma(2), dma(NSMEAR + 2, 4), dma(copies), dma(copies),
        ],
        compiler_params=pltpu.CompilerParams(
            collective_id=0, has_side_effects=True, vmem_limit_bytes=48 * 1024 * 1024
        ),
    )(
        source_sites.reshape(4),
        links.reshape(72, rows, lanes),
        guess.reshape(12, 24, rows, lanes),
    )
    return sol.reshape(guess.shape), res.reshape(guess.shape)


def solution(mesh):
    sizes = tuple(mesh.shape[axis] for axis in AXES)
    fields = P(None, None, None, None, "ta", "xy", "gz")
    return jax.shard_map(
        functools.partial(on_device, sizes),
        mesh=mesh,
        in_specs=(fields, fields, P("ta", "xy", "gz", None)),
        out_specs=(fields, fields),
        check_vma=False,
    )
```

```python
import functools

import jax
import jax.numpy as jnp
from jax import lax
from jax.experimental import pallas as pl
from jax.experimental.pallas import tpu as pltpu
from jax.sharding import PartitionSpec as P

LX = 32
NSMEAR = 8
HOP = 0.12
PAIRS = 6
EDGE_CHUNK = 3
TIME_CHUNK = 1
MESH = pl.DeviceIdType.MESH
AXES = ("xy", "gz", "ta")

E_ROWS = (
    ((1, -1j), (0, -1j)),
    ((1, -1), (0, 1)),
    ((0, -1j), (1, 1j)),
    ((0, 1), (1, 1)),
)


def times(coef, z):
    re, im = z
    if coef == 1:
        return (1, re), (1, im)
    if coef == -1:
        return (-1, re), (-1, im)
    if coef == 1j:
        return (-1, im), (1, re)
    return (1, im), (-1, re)


def add_term(z, coef, other):
    out = []
    for base, (sign, term) in zip(z, times(coef, other)):
        out.append(base + term if sign > 0 else base - term)
    return tuple(out)


def project(f, mu, parity):
    half = []
    for row in range(2):
        column, coef = E_ROWS[mu][row]
        half.append([add_term(f[row][a], parity * coef, f[2 + column][a]) for a in range(3)])
    return half


def lift_add(total, h, mu, parity):
    for row in range(2):
        column, coef = E_ROWS[mu][row]
        for a in range(3):
            total[row][a] = add_term(total[row][a], 1, h[row][a])
            low = parity * complex(coef).conjugate()
            total[2 + column][a] = add_term(total[2 + column][a], low, h[row][a])


def link_times(link, mu, vectors, adjoint):
    def entry(a, b):
        if adjoint:
            a, b = b, a
        base = mu * 18 + a * 3 + b
        return link[base], link[base + 9]

    out = [[None] * 3 for _ in vectors]
    for a in range(3):
        totals = [None] * len(vectors)
        for b in range(3):
            ur, ui = entry(a, b)
            for k, vec in enumerate(vectors):
                re, im = vec[b]
                if adjoint:
                    tr, ti = ur * re + ui * im, ur * im - ui * re
                else:
                    tr, ti = ur * re - ui * im, ur * im + ui * re
                old = totals[k]
                totals[k] = (tr, ti) if old is None else (old[0] + tr, old[1] + ti)
        for k in range(len(vectors)):
            out[k][a] = totals[k]
    return out


def flat(vectors):
    return [vec[a][part] for part in range(2) for vec in vectors for a in range(3)]


def unflat(items, count):
    return [
        [(items[k * 3 + a], items[3 * count + k * 3 + a]) for a in range(3)] for k in range(count)
    ]


class Shifts:
    def __init__(self):
        row = lax.broadcasted_iota(jnp.int32, (8, 128), 0)
        lane = lax.broadcasted_iota(jnp.int32, (8, 128), 1)
        self.low = row < 4
        self.lane = lane
        self.place = ([row % 4 == k for k in range(4)], [lane // LX == k for k in range(4)])
        self.x_first = lane % LX == 0
        self.x_last = lane % LX == LX - 1
        self.unit = ((0, 1, 8), (1, LX, 128))

    def roll(self, v, kind, steps):
        axis, unit, size = self.unit[kind]
        amount = (steps * unit) % size
        return v if amount == 0 else pltpu.roll(v, amount, axis)

    def pack(self, items, kind, ahead):
        packed = []
        for g in range(0, len(items), 4):
            out = None
            for k in range(4):
                v = self.roll(items[g + k], kind, k if ahead else k - 3)
                out = v if out is None else jnp.where(self.place[kind][k], v, out)
            packed.append(out)
        return packed

    def shift(self, items, packed, kind, ahead):
        outs = []
        for i, v in enumerate(items):
            got = packed[i // 4]
            k = i % 4
            if ahead:
                moved = self.roll(v, kind, -1)
                outs.append(jnp.where(self.place[kind][3], self.roll(got, kind, 3 - k), moved))
            else:
                moved = self.roll(v, kind, 1)
                outs.append(jnp.where(self.place[kind][0], self.roll(got, kind, -k), moved))
        return outs

    def along_x(self, items, ahead):
        outs = []
        for v in items:
            if ahead:
                a, b = pltpu.roll(v, 127, 1), pltpu.roll(v, LX - 1, 1)
                outs.append(jnp.where(self.x_last, b, a))
            else:
                a, b = pltpu.roll(v, 1, 1), pltpu.roll(v, 129 - LX, 1)
                outs.append(jnp.where(self.x_first, b, a))
        return outs


def kernel(
    sizes, sites_ref, links_ref, guess_ref, sol_ref, res_ref,
    link, guess, field_a, field_b, search, acc, right, carried,
    edge_out, edge_in, time_out, time_in, sm_out, sm_in, smt_out, smt_in,
    red_out, red_in, sums,
    edge_sem, time_sem, w_send, sm_sem, smt_sem, s_send, red_sem, r_send,
):
    n_of = dict(zip(AXES, sizes))
    me = {axis: lax.axis_index(axis) for axis in AXES}

    def peer(axis, step):
        return {axis: lax.rem(me[axis] + step + n_of[axis], n_of[axis])}

    barrier = pltpu.get_barrier_semaphore()
    for axis in AXES:
        for k in range(1, n_of[axis]):
            pl.semaphore_signal(barrier, inc=1, device_id=peer(axis, k), device_id_type=MESH)

    sh = Shifts()

    sign = jnp.where(me["ta"] == n_of["ta"] - 1, -1.0, 1.0).astype(jnp.float32)
    for i in range(72):
        v = links_ref[i]
        if i >= 54:
            v = v * sign
        link[i, 0:4, :] = v
        link[i, 4:8, :] = v

    def rhs_of(p):
        first = jnp.where(p < 4, 3 * p, 6 * p - 22)
        second = jnp.where(p < 4, 3 * p + 1, 6 * p - 19)
        return first, second

    def load_guess(p, _):
        first, second = rhs_of(p)
        for i in range(24):
            guess[p, i, 0:4, :] = guess_ref[first, i]
            guess[p, i, 4:8, :] = guess_ref[second, i]
        return _

    lax.fori_loop(0, PAIRS, load_guess, 0)
    pl.semaphore_wait(barrier, sum(n - 1 for n in sizes))

    def part_of(p, chunk):
        return pl.ds(p, chunk)

    def start_last(make, w, d, p, chunk):
        if chunk == 1:
            make(w, d, p).start()
        else:
            @pl.when(lax.rem(p, chunk) == chunk - 1)
            def _():
                make(w, d, p - (chunk - 1)).start()

    def await_first(make, w, p, chunk, dirs):
        def wait():
            for d in dirs:
                make(w, d, p).wait_recv()
        if chunk == 1:
            wait()
        else:
            pl.when(lax.rem(p, chunk) == 0)(wait)

    def edge_copy(w, d, p):
        axis, step = (("xy", -1), ("xy", 1), ("gz", -1), ("gz", 1))[d]
        return pltpu.make_async_remote_copy(
            src_ref=edge_out.at[w, d, part_of(p, EDGE_CHUNK)], dst_ref=edge_in.at[w, d, part_of(p, EDGE_CHUNK)],
            send_sem=w_send.at[w, d, p], recv_sem=edge_sem.at[w, d, p],
            device_id=peer(axis, step), device_id_type=MESH,
        )

    def time_copy(w, d, p):
        return pltpu.make_async_remote_copy(
            src_ref=time_out.at[w, d, part_of(p, TIME_CHUNK)], dst_ref=time_in.at[w, d, part_of(p, TIME_CHUNK)],
            send_sem=w_send.at[w, 4 + d, p], recv_sem=time_sem.at[w, d, p],
            device_id=peer("ta", (-1, 1)[d]), device_id_type=MESH,
        )

    def load_field(ref, p):
        return unflat([ref[p, i] for i in range(24)], 4)

    def send_body(f, w, p, par):
        for i, v in enumerate(flat(project(f, 3, -par))):
            time_out[w, 0, p, i] = v
        start_last(time_copy, w, 0, p, TIME_CHUNK)
        for i, v in enumerate(flat(link_times(link, 3, project(f, 3, par), True))):
            time_out[w, 1, p, i] = v
        start_last(time_copy, w, 1, p, TIME_CHUNK)
        for kind, mu in ((0, 1), (1, 2)):
            for i, v in enumerate(sh.pack(flat(project(f, mu, -par)), kind, True)):
                edge_out[w, 2 * kind, p, i] = v
            start_last(edge_copy, w, 2 * kind, p, EDGE_CHUNK)
            behind = flat(link_times(link, mu, project(f, mu, par), True))
            for i, v in enumerate(behind):
                carried[kind, p, i] = v
            for i, v in enumerate(sh.pack(behind, kind, False)):
                edge_out[w, 2 * kind + 1, p, i] = v
            start_last(edge_copy, w, 2 * kind + 1, p, EDGE_CHUNK)

    def interior(src, par):
        def body(p, _):
            f = load_field(src, p)
            zero = jnp.zeros((8, 128), jnp.float32)
            total = [[(zero, zero)] * 3 for _ in range(4)]
            ahead = unflat(sh.along_x(flat(project(f, 0, -par)), True), 2)
            lift_add(total, link_times(link, 0, ahead, False), 0, -par)
            behind = flat(link_times(link, 0, project(f, 0, par), True))
            lift_add(total, unflat(sh.along_x(behind, False), 2), 0, par)
            for i, v in enumerate(flat(total)):
                acc[p, i] = v
            return _
        lax.fori_loop(0, PAIRS, body, 0)

    def receive_body(src, w, p, par):
        await_first(edge_copy, w, p, EDGE_CHUNK, range(4))
        await_first(time_copy, w, p, TIME_CHUNK, range(2))
        f = load_field(src, p)
        total = load_field(acc, p)
        for kind, mu in ((0, 1), (1, 2)):
            got = [edge_in[w, 2 * kind, p, i] for i in range(3)]
            ahead = unflat(sh.shift(flat(project(f, mu, -par)), got, kind, True), 2)
            lift_add(total, link_times(link, mu, ahead, False), mu, -par)
            got = [edge_in[w, 2 * kind + 1, p, i] for i in range(3)]
            local = [carried[kind, p, i] for i in range(12)]
            lift_add(total, unflat(sh.shift(local, got, kind, False), 2), mu, par)
        ahead = unflat([time_in[w, 0, p, i] for i in range(12)], 2)
        lift_add(total, link_times(link, 3, ahead, False), 3, -par)
        lift_add(total, unflat([time_in[w, 1, p, i] for i in range(12)], 2), 3, par)
        return [a - HOP * b for a, b in zip(flat(f), flat(total))]

    def sm_copy(step, d):
        axis, hop = (("xy", -1), ("xy", 1), ("gz", -1), ("gz", 1))[d]
        return pltpu.make_async_remote_copy(
            src_ref=sm_out.at[step, d], dst_ref=sm_in.at[step, d],
            send_sem=s_send.at[step, d], recv_sem=sm_sem.at[step, d],
            device_id=peer(axis, hop), device_id_type=MESH,
        )

    def smt_copy(d):
        return pltpu.make_async_remote_copy(
            src_ref=smt_out.at[d], dst_ref=smt_in.at[d],
            send_sem=s_send.at[NSMEAR + 1, d], recv_sem=smt_sem.at[d],
            device_id=peer("ta", (-1, 1)[d]), device_id_type=MESH,
        )

    def colour_hops(items, step, beside):
        vectors = unflat(items, 2)
        behinds = []
        for kind, mu in ((0, 1), (1, 2)):
            for i, v in enumerate(sh.pack(items, kind, True)):
                sm_out[step, 2 * kind, i] = v
            sm_copy(step, 2 * kind).start()
            behind = flat(link_times(link, mu, vectors, True))
            behinds.append(behind)
            for i, v in enumerate(sh.pack(behind, kind, False)):
                sm_out[step, 2 * kind + 1, i] = v
            sm_copy(step, 2 * kind + 1).start()
        for body, first, end in beside:
            if body in (interior_guess, interior_field):
                body()
            else:
                lax.fori_loop(first, end, body, 0)
        aheads_out = [flat(link_times(link, 0, unflat(sh.along_x(items, True), 2), False))]
        behinds_out = [sh.along_x(flat(link_times(link, 0, vectors, True)), False)]
        for kind, mu in ((0, 1), (1, 2)):
            sm_copy(step, 2 * kind).wait_recv()
            got = [sm_in[step, 2 * kind, i] for i in range(3)]
            ahead = unflat(sh.shift(items, got, kind, True), 2)
            aheads_out.append(flat(link_times(link, mu, ahead, False)))
            sm_copy(step, 2 * kind + 1).wait_recv()
            got = [sm_in[step, 2 * kind + 1, i] for i in range(3)]
            behinds_out.append(sh.shift(behinds[kind], got, kind, False))
        return aheads_out, behinds_out

    def smear_step(step, items, beside):
        aheads, behinds = colour_hops(list(items), step, beside)
        out = []
        for i, v in enumerate(items):
            total = None
            for part in aheads + behinds:
                total = part[i] if total is None else total + part[i]
            out.append((v + 0.25 * total) * 0.5)
        return tuple(out)

    def start_right(items):
        for i, v in enumerate(items):
            smt_out[0, i] = v
        smt_copy(0).start()
        for i, v in enumerate(flat(link_times(link, 3, unflat(items, 2), True))):
            smt_out[1, i] = v
        smt_copy(1).start()

    def finish_right(items, beside):
        aheads, behinds = colour_hops(items, NSMEAR, beside)
        smt_copy(0).wait_recv()
        got = unflat([smt_in[0, i] for i in range(12)], 2)
        aheads.append(flat(link_times(link, 3, got, False)))
        smt_copy(1).wait_recv()
        behinds.append([smt_in[1, i] for i in range(12)])
        diag = []
        for i, v in enumerate(items):
            total = None
            for part in aheads + behinds:
                total = part[i] if total is None else total + part[i]
            diag.append(v - HOP * total)
        diag = unflat(diag, 2)
        gs = [
            unflat([-HOP * (a - b) for a, b in zip(aheads[mu], behinds[mu])], 2)
            for mu in range(4)
        ]
        zero = jnp.zeros((8, 128), jnp.float32)

        def block(s2, s, q, a):
            if s2 == s:
                return diag[q][a]
            if s2 // 2 == s // 2:
                return (zero, zero)
            out = (zero, zero)
            for mu in range(4):
                for row in range(2):
                    column, coef = E_ROWS[mu][row]
                    if s2 < 2 and row == s2 and column == s - 2:
                        out = add_term(out, coef, gs[mu][q][a])
                    if s2 >= 2 and column == s2 - 2 and row == s:
                        out = add_term(out, complex(coef).conjugate(), gs[mu][q][a])
            return out

        for s2 in range(4):
            for a in range(3):
                column = [block(s2, s, 0, a) for s in range(4)]
                lone = [block(s2, s, 1, a) for s in range(4)]
                for part in range(2):
                    i = part * 12 + s2 * 3 + a
                    for s in range(4):
                        right[s, i] = column[s][part]
                    right[4, i] = jnp.where(sh.low, lone[0][part], lone[1][part])
                    right[5, i] = jnp.where(sh.low, lone[2][part], lone[3][part])

    def first_send(p, _):
        send_body(load_field(guess, p), 0, p, 1)
        return _

    row = lax.broadcasted_iota(jnp.int32, (8, 128), 0)
    hit = (row % 4 == sites_ref[1]) & (sh.lane == sites_ref[2] * LX + sites_ref[3])
    hit = hit & (sites_ref[0] == 0)
    one = jnp.where(hit, 1.0, 0.0).astype(jnp.float32)
    zero = jnp.zeros((8, 128), jnp.float32)
    upper, lower = jnp.where(sh.low, one, 0.0), jnp.where(sh.low, 0.0, one)
    items = tuple(flat([
        [(upper, zero), (lower, zero), (zero, zero)],
        [(zero, zero), (zero, zero), (one, zero)],
    ]))

    def interior_guess():
        interior(guess, 1)

    def interior_field():
        interior(field_a, -1)

    def second(p, _):
        out = receive_body(guess, 0, p, 1)
        for i, v in enumerate(out):
            field_a[p, i] = v
        send_body(unflat(out, 4), 1, p, -1)
        return _

    def normal(p, _):
        for i, v in enumerate(receive_body(field_a, 1, p, -1)):
            search[p, i] = v
        return _

    def third(p, _):
        out = [right[p, i] - search[p, i] for i in range(24)]
        total = None
        for i, v in enumerate(out):
            search[p, i] = v
            total = v * v if total is None else total + v * v
        sums[p] = total
        send_body(unflat(out, 4), 2, p, 1)
        return _

    beside = {
        0: [(first_send, 0, 6)],
        1: [(interior_guess, 0, 0)],
        2: [(second, 0, 2)],
        3: [(second, 2, 4)],
        4: [(second, 4, 6)],
        5: [(interior_field, 0, 0)],
        6: [(normal, 0, 2)],
        7: [(normal, 2, 4)],
        8: [(normal, 4, 6)],
    }
    for step in range(NSMEAR):
        items = smear_step(step, items, beside.get(step, []))
    items = list(items)
    start_right(items)
    finish_right(items, beside[NSMEAR])

    lax.fori_loop(0, PAIRS, third, 0)
    interior(search, 1)

    def fourth(p, _):
        out = receive_body(search, 2, p, 1)
        total = None
        for i, v in enumerate(out):
            field_b[p, i] = v
            total = v * v if total is None else total + v * v
        sums[PAIRS + p] = total
        send_body(unflat(out, 4), 3, p, -1)
        return _

    lax.fori_loop(0, PAIRS, fourth, 0)

    mine = jnp.zeros((8, 128), jnp.float32)
    for k in range(2 * PAIRS):
        mine = jnp.where(sh.lane == k, jnp.sum(sums[k], axis=1, keepdims=True), mine)
    slot = 0
    done_interior = False
    for stage, axis in enumerate(AXES):
        red_out[stage] = mine
        copies = []
        for k in range(1, n_of[axis]):
            copy = pltpu.make_async_remote_copy(
                src_ref=red_out.at[stage], dst_ref=red_in.at[slot],
                send_sem=r_send.at[slot], recv_sem=red_sem.at[slot],
                device_id=peer(axis, k), device_id_type=MESH,
            )
            copy.start()
            copies.append((copy, slot))
            slot += 1
        if not done_interior:
            interior(field_b, -1)
            done_interior = True
        for copy, place in copies:
            copy.wait()
            mine = mine + red_in[place]
    top = jnp.sum(mine[0:4], axis=0, keepdims=True)
    bottom = jnp.sum(mine[4:8], axis=0, keepdims=True)
    both = jnp.where(sh.low, top, bottom)
    curvature = pltpu.roll(both, 128 - PAIRS, 1)
    steps = both / jnp.where(sh.lane < PAIRS, curvature, 1.0)

    def last(p, _):
        out = receive_body(field_b, 3, p, -1)
        length = jnp.sum(jnp.where(sh.lane == p, steps, 0.0), axis=1, keepdims=True)
        first, second_rhs = rhs_of(p)
        for i, v in enumerate(out):
            s = search[p, i]
            res = s - length * v
            sol = guess[p, i] + length * s
            res_ref[first, i] = res[0:4]
            res_ref[second_rhs, i] = res[4:8]
            sol_ref[first, i] = sol[0:4]
            sol_ref[second_rhs, i] = sol[4:8]
        return _

    lax.fori_loop(0, PAIRS, last, 0)

    def drain(w, _):
        for p in range(0, PAIRS, EDGE_CHUNK):
            for d in range(4):
                edge_copy(w, d, p).wait_send()
        for p in range(0, PAIRS, TIME_CHUNK):
            for d in range(2):
                time_copy(w, d, p).wait_send()
        return _

    lax.fori_loop(0, 4, drain, 0)

    def drain_s(step, _):
        for d in range(4):
            sm_copy(step, d).wait_send()
        return _

    lax.fori_loop(0, NSMEAR + 1, drain_s, 0)
    for d in range(2):
        smt_copy(d).wait_send()


def on_device(sizes, links, guess, source_sites):
    rows, lanes = guess.shape[-2:]
    f32 = jnp.float32
    copies = sum(n - 1 for n in sizes)
    tile = (8, lanes)
    vm = lambda *shape: pltpu.VMEM(shape + tile, f32)
    dma = lambda *shape: pltpu.SemaphoreType.DMA(shape)
    out = jax.ShapeDtypeStruct((12, 24, rows, lanes), f32)
    sol, res = pl.pallas_call(
        functools.partial(kernel, sizes),
        out_shape=(out, out),
        in_specs=[
            pl.BlockSpec(memory_space=pltpu.SMEM),
            pl.BlockSpec(memory_space=pltpu.VMEM),
            pl.BlockSpec(memory_space=pltpu.VMEM),
        ],
        out_specs=(pl.BlockSpec(memory_space=pltpu.VMEM), pl.BlockSpec(memory_space=pltpu.VMEM)),
        scratch_shapes=[
            vm(72), vm(PAIRS, 24), vm(PAIRS, 24), vm(PAIRS, 24), vm(PAIRS, 24), vm(PAIRS, 24),
            vm(PAIRS, 24), vm(2, PAIRS, 12),
            vm(4, 4, PAIRS, 3), vm(4, 4, PAIRS, 3), vm(4, 2, PAIRS, 12), vm(4, 2, PAIRS, 12),
            vm(NSMEAR + 1, 4, 3), vm(NSMEAR + 1, 4, 3), vm(2, 12), vm(2, 12),
            vm(3), vm(copies), vm(2 * PAIRS),
            dma(4, 4, PAIRS), dma(4, 2, PAIRS), dma(4, 6, PAIRS),
            dma(NSMEAR + 1, 4), dma(2), dma(NSMEAR + 2, 4), dma(copies), dma(copies),
        ],
        compiler_params=pltpu.CompilerParams(
            collective_id=0, has_side_effects=True, vmem_limit_bytes=48 * 1024 * 1024
        ),
    )(
        source_sites.reshape(4),
        links.reshape(72, rows, lanes),
        guess.reshape(12, 24, rows, lanes),
    )
    return sol.reshape(guess.shape), res.reshape(guess.shape)


def solution(mesh):
    sizes = tuple(mesh.shape[axis] for axis in AXES)
    fields = P(None, None, None, None, "ta", "xy", "gz")
    return jax.shard_map(
        functools.partial(on_device, sizes),
        mesh=mesh,
        in_specs=(fields, fields, P("ta", "xy", "gz", None)),
        out_specs=(fields, fields),
        check_vma=False,
    )
```

```python
import functools

import jax
import jax.numpy as jnp
from jax import lax
from jax.experimental import pallas as pl
from jax.experimental.pallas import tpu as pltpu
from jax.sharding import PartitionSpec as P

LX = 32
NSMEAR = 8
HOP = 0.12
PAIRS = 6
EDGE_CHUNK = 3
TIME_CHUNK = 1
MESH = pl.DeviceIdType.MESH
AXES = ("xy", "gz", "ta")

E_ROWS = (
    ((1, -1j), (0, -1j)),
    ((1, -1), (0, 1)),
    ((0, -1j), (1, 1j)),
    ((0, 1), (1, 1)),
)


def times(coef, z):
    re, im = z
    if coef == 1:
        return (1, re), (1, im)
    if coef == -1:
        return (-1, re), (-1, im)
    if coef == 1j:
        return (-1, im), (1, re)
    return (1, im), (-1, re)


def add_term(z, coef, other):
    out = []
    for base, (sign, term) in zip(z, times(coef, other)):
        out.append(base + term if sign > 0 else base - term)
    return tuple(out)


def project(f, mu, parity):
    half = []
    for row in range(2):
        column, coef = E_ROWS[mu][row]
        half.append([add_term(f[row][a], parity * coef, f[2 + column][a]) for a in range(3)])
    return half


def lift_add(total, h, mu, parity):
    for row in range(2):
        column, coef = E_ROWS[mu][row]
        for a in range(3):
            total[row][a] = add_term(total[row][a], 1, h[row][a])
            low = parity * complex(coef).conjugate()
            total[2 + column][a] = add_term(total[2 + column][a], low, h[row][a])


def link_times(link, mu, vectors, adjoint):
    def entry(a, b):
        if adjoint:
            a, b = b, a
        base = mu * 18 + a * 3 + b
        return link[base], link[base + 9]

    out = [[None] * 3 for _ in vectors]
    for a in range(3):
        totals = [None] * len(vectors)
        for b in range(3):
            ur, ui = entry(a, b)
            for k, vec in enumerate(vectors):
                re, im = vec[b]
                if adjoint:
                    tr, ti = ur * re + ui * im, ur * im - ui * re
                else:
                    tr, ti = ur * re - ui * im, ur * im + ui * re
                old = totals[k]
                totals[k] = (tr, ti) if old is None else (old[0] + tr, old[1] + ti)
        for k in range(len(vectors)):
            out[k][a] = totals[k]
    return out


def flat(vectors):
    return [vec[a][part] for part in range(2) for vec in vectors for a in range(3)]


def unflat(items, count):
    return [
        [(items[k * 3 + a], items[3 * count + k * 3 + a]) for a in range(3)] for k in range(count)
    ]


class Shifts:
    def __init__(self):
        row = lax.broadcasted_iota(jnp.int32, (8, 128), 0)
        lane = lax.broadcasted_iota(jnp.int32, (8, 128), 1)
        self.low = row < 4
        self.lane = lane
        self.place = ([row % 4 == k for k in range(4)], [lane // LX == k for k in range(4)])
        self.x_first = lane % LX == 0
        self.x_last = lane % LX == LX - 1
        self.unit = ((0, 1, 8), (1, LX, 128))

    def roll(self, v, kind, steps):
        axis, unit, size = self.unit[kind]
        amount = (steps * unit) % size
        return v if amount == 0 else pltpu.roll(v, amount, axis)

    def pack(self, items, kind, ahead):
        packed = []
        for g in range(0, len(items), 4):
            out = None
            for k in range(4):
                v = self.roll(items[g + k], kind, k if ahead else k - 3)
                out = v if out is None else jnp.where(self.place[kind][k], v, out)
            packed.append(out)
        return packed

    def shift(self, items, packed, kind, ahead):
        outs = []
        for i, v in enumerate(items):
            got = packed[i // 4]
            k = i % 4
            if ahead:
                moved = self.roll(v, kind, -1)
                outs.append(jnp.where(self.place[kind][3], self.roll(got, kind, 3 - k), moved))
            else:
                moved = self.roll(v, kind, 1)
                outs.append(jnp.where(self.place[kind][0], self.roll(got, kind, -k), moved))
        return outs

    def along_x(self, items, ahead):
        outs = []
        for v in items:
            if ahead:
                a, b = pltpu.roll(v, 127, 1), pltpu.roll(v, LX - 1, 1)
                outs.append(jnp.where(self.x_last, b, a))
            else:
                a, b = pltpu.roll(v, 1, 1), pltpu.roll(v, 129 - LX, 1)
                outs.append(jnp.where(self.x_first, b, a))
        return outs


def kernel(
    sizes, sites_ref, links_ref, guess_ref, sol_ref, res_ref,
    link, guess, field_a, field_b, search, acc, right, carried,
    edge_out, edge_in, time_out, time_in, sm_out, sm_in, smt_out, smt_in,
    red_out, red_in, sums,
    edge_sem, time_sem, w_send, sm_sem, smt_sem, s_send, red_sem, r_send,
):
    n_of = dict(zip(AXES, sizes))
    me = {axis: lax.axis_index(axis) for axis in AXES}

    def peer(axis, step):
        return {axis: lax.rem(me[axis] + step + n_of[axis], n_of[axis])}

    barrier = pltpu.get_barrier_semaphore()
    for axis in AXES:
        for k in range(1, n_of[axis]):
            pl.semaphore_signal(barrier, inc=1, device_id=peer(axis, k), device_id_type=MESH)

    sh = Shifts()

    sign = jnp.where(me["ta"] == n_of["ta"] - 1, -1.0, 1.0).astype(jnp.float32)
    for i in range(72):
        v = links_ref[i]
        if i >= 54:
            v = v * sign
        link[i, 0:4, :] = v
        link[i, 4:8, :] = v

    def rhs_of(p):
        first = jnp.where(p < 4, 3 * p, 6 * p - 22)
        second = jnp.where(p < 4, 3 * p + 1, 6 * p - 19)
        return first, second

    def load_guess(p, _):
        first, second = rhs_of(p)
        for i in range(24):
            guess[p, i, 0:4, :] = guess_ref[first, i]
            guess[p, i, 4:8, :] = guess_ref[second, i]
        return _

    lax.fori_loop(0, PAIRS, load_guess, 0)
    pl.semaphore_wait(barrier, sum(n - 1 for n in sizes))

    def part_of(p, chunk):
        return pl.ds(p, chunk)

    def start_last(make, w, d, p, chunk):
        if chunk == 1:
            make(w, d, p).start()
        else:
            @pl.when(lax.rem(p, chunk) == chunk - 1)
            def _():
                make(w, d, p - (chunk - 1)).start()

    def await_first(make, w, p, chunk, dirs):
        def wait():
            for d in dirs:
                make(w, d, p).wait_recv()
        if chunk == 1:
            wait()
        else:
            pl.when(lax.rem(p, chunk) == 0)(wait)

    def edge_copy(w, d, p):
        axis, step = (("xy", -1), ("xy", 1), ("gz", -1), ("gz", 1))[d]
        return pltpu.make_async_remote_copy(
            src_ref=edge_out.at[w, d, part_of(p, EDGE_CHUNK)], dst_ref=edge_in.at[w, d, part_of(p, EDGE_CHUNK)],
            send_sem=w_send.at[w, d, p], recv_sem=edge_sem.at[w, d, p],
            device_id=peer(axis, step), device_id_type=MESH,
        )

    def time_copy(w, d, p):
        return pltpu.make_async_remote_copy(
            src_ref=time_out.at[w, d, part_of(p, TIME_CHUNK)], dst_ref=time_in.at[w, d, part_of(p, TIME_CHUNK)],
            send_sem=w_send.at[w, 4 + d, p], recv_sem=time_sem.at[w, d, p],
            device_id=peer("ta", (-1, 1)[d]), device_id_type=MESH,
        )

    def load_field(ref, p):
        return unflat([ref[p, i] for i in range(24)], 4)

    def send_body(f, w, p, par):
        for i, v in enumerate(flat(project(f, 3, -par))):
            time_out[w, 0, p, i] = v
        start_last(time_copy, w, 0, p, TIME_CHUNK)
        for i, v in enumerate(flat(link_times(link, 3, project(f, 3, par), True))):
            time_out[w, 1, p, i] = v
        start_last(time_copy, w, 1, p, TIME_CHUNK)
        for kind, mu in ((0, 1), (1, 2)):
            for i, v in enumerate(sh.pack(flat(project(f, mu, -par)), kind, True)):
                edge_out[w, 2 * kind, p, i] = v
            start_last(edge_copy, w, 2 * kind, p, EDGE_CHUNK)
            behind = flat(link_times(link, mu, project(f, mu, par), True))
            for i, v in enumerate(behind):
                carried[kind, p, i] = v
            for i, v in enumerate(sh.pack(behind, kind, False)):
                edge_out[w, 2 * kind + 1, p, i] = v
            start_last(edge_copy, w, 2 * kind + 1, p, EDGE_CHUNK)

    def interior(src, par):
        def body(p, _):
            f = load_field(src, p)
            zero = jnp.zeros((8, 128), jnp.float32)
            total = [[(zero, zero)] * 3 for _ in range(4)]
            ahead = unflat(sh.along_x(flat(project(f, 0, -par)), True), 2)
            lift_add(total, link_times(link, 0, ahead, False), 0, -par)
            behind = flat(link_times(link, 0, project(f, 0, par), True))
            lift_add(total, unflat(sh.along_x(behind, False), 2), 0, par)
            for i, v in enumerate(flat(total)):
                acc[p, i] = v
            return _
        lax.fori_loop(0, PAIRS, body, 0)

    def receive_body(src, w, p, par):
        await_first(edge_copy, w, p, EDGE_CHUNK, range(4))
        await_first(time_copy, w, p, TIME_CHUNK, range(2))
        f = load_field(src, p)
        total = load_field(acc, p)
        for kind, mu in ((0, 1), (1, 2)):
            got = [edge_in[w, 2 * kind, p, i] for i in range(3)]
            ahead = unflat(sh.shift(flat(project(f, mu, -par)), got, kind, True), 2)
            lift_add(total, link_times(link, mu, ahead, False), mu, -par)
            got = [edge_in[w, 2 * kind + 1, p, i] for i in range(3)]
            local = [carried[kind, p, i] for i in range(12)]
            lift_add(total, unflat(sh.shift(local, got, kind, False), 2), mu, par)
        ahead = unflat([time_in[w, 0, p, i] for i in range(12)], 2)
        lift_add(total, link_times(link, 3, ahead, False), 3, -par)
        lift_add(total, unflat([time_in[w, 1, p, i] for i in range(12)], 2), 3, par)
        return [a - HOP * b for a, b in zip(flat(f), flat(total))]

    def sm_copy(step, d):
        axis, hop = (("xy", -1), ("xy", 1), ("gz", -1), ("gz", 1))[d]
        return pltpu.make_async_remote_copy(
            src_ref=sm_out.at[step, d], dst_ref=sm_in.at[step, d],
            send_sem=s_send.at[step, d], recv_sem=sm_sem.at[step, d],
            device_id=peer(axis, hop), device_id_type=MESH,
        )

    def smt_copy(d):
        return pltpu.make_async_remote_copy(
            src_ref=smt_out.at[d], dst_ref=smt_in.at[d],
            send_sem=s_send.at[NSMEAR + 1, d], recv_sem=smt_sem.at[d],
            device_id=peer("ta", (-1, 1)[d]), device_id_type=MESH,
        )

    def colour_hops(items, step, beside):
        vectors = unflat(items, 2)
        behinds = []
        for kind in range(2):
            for i, v in enumerate(sh.pack(items, kind, True)):
                sm_out[step, 2 * kind, i] = v
            sm_copy(step, 2 * kind).start()
        for kind, mu in ((0, 1), (1, 2)):
            behind = flat(link_times(link, mu, vectors, True))
            behinds.append(behind)
            for i, v in enumerate(sh.pack(behind, kind, False)):
                sm_out[step, 2 * kind + 1, i] = v
            sm_copy(step, 2 * kind + 1).start()
        for body, first, end in beside:
            if body in (interior_guess, interior_field):
                body()
            else:
                lax.fori_loop(first, end, body, 0)
        aheads_out = [flat(link_times(link, 0, unflat(sh.along_x(items, True), 2), False))]
        behinds_out = [sh.along_x(flat(link_times(link, 0, vectors, True)), False)]
        for kind, mu in ((0, 1), (1, 2)):
            sm_copy(step, 2 * kind).wait_recv()
            got = [sm_in[step, 2 * kind, i] for i in range(3)]
            ahead = unflat(sh.shift(items, got, kind, True), 2)
            aheads_out.append(flat(link_times(link, mu, ahead, False)))
            sm_copy(step, 2 * kind + 1).wait_recv()
            got = [sm_in[step, 2 * kind + 1, i] for i in range(3)]
            behinds_out.append(sh.shift(behinds[kind], got, kind, False))
        return aheads_out, behinds_out

    def smear_step(step, items, beside):
        aheads, behinds = colour_hops(list(items), step, beside)
        out = []
        for i, v in enumerate(items):
            total = None
            for part in aheads + behinds:
                total = part[i] if total is None else total + part[i]
            out.append((v + 0.25 * total) * 0.5)
        return tuple(out)

    def start_right(items):
        for i, v in enumerate(items):
            smt_out[0, i] = v
        smt_copy(0).start()
        for i, v in enumerate(flat(link_times(link, 3, unflat(items, 2), True))):
            smt_out[1, i] = v
        smt_copy(1).start()

    def finish_right(items, beside):
        aheads, behinds = colour_hops(items, NSMEAR, beside)
        smt_copy(0).wait_recv()
        got = unflat([smt_in[0, i] for i in range(12)], 2)
        aheads.append(flat(link_times(link, 3, got, False)))
        smt_copy(1).wait_recv()
        behinds.append([smt_in[1, i] for i in range(12)])
        diag = []
        for i, v in enumerate(items):
            total = None
            for part in aheads + behinds:
                total = part[i] if total is None else total + part[i]
            diag.append(v - HOP * total)
        diag = unflat(diag, 2)
        gs = [
            unflat([-HOP * (a - b) for a, b in zip(aheads[mu], behinds[mu])], 2)
            for mu in range(4)
        ]
        zero = jnp.zeros((8, 128), jnp.float32)

        def block(s2, s, q, a):
            if s2 == s:
                return diag[q][a]
            if s2 // 2 == s // 2:
                return (zero, zero)
            out = (zero, zero)
            for mu in range(4):
                for row in range(2):
                    column, coef = E_ROWS[mu][row]
                    if s2 < 2 and row == s2 and column == s - 2:
                        out = add_term(out, coef, gs[mu][q][a])
                    if s2 >= 2 and column == s2 - 2 and row == s:
                        out = add_term(out, complex(coef).conjugate(), gs[mu][q][a])
            return out

        for s2 in range(4):
            for a in range(3):
                column = [block(s2, s, 0, a) for s in range(4)]
                lone = [block(s2, s, 1, a) for s in range(4)]
                for part in range(2):
                    i = part * 12 + s2 * 3 + a
                    for s in range(4):
                        right[s, i] = column[s][part]
                    right[4, i] = jnp.where(sh.low, lone[0][part], lone[1][part])
                    right[5, i] = jnp.where(sh.low, lone[2][part], lone[3][part])

    def first_send(p, _):
        send_body(load_field(guess, p), 0, p, 1)
        return _

    row = lax.broadcasted_iota(jnp.int32, (8, 128), 0)
    hit = (row % 4 == sites_ref[1]) & (sh.lane == sites_ref[2] * LX + sites_ref[3])
    hit = hit & (sites_ref[0] == 0)
    one = jnp.where(hit, 1.0, 0.0).astype(jnp.float32)
    zero = jnp.zeros((8, 128), jnp.float32)
    upper, lower = jnp.where(sh.low, one, 0.0), jnp.where(sh.low, 0.0, one)
    items = tuple(flat([
        [(upper, zero), (lower, zero), (zero, zero)],
        [(zero, zero), (zero, zero), (one, zero)],
    ]))

    def interior_guess():
        interior(guess, 1)

    def interior_field():
        interior(field_a, -1)

    def second(p, _):
        out = receive_body(guess, 0, p, 1)
        for i, v in enumerate(out):
            field_a[p, i] = v
        send_body(unflat(out, 4), 1, p, -1)
        return _

    def normal(p, _):
        for i, v in enumerate(receive_body(field_a, 1, p, -1)):
            search[p, i] = v
        return _

    def third(p, _):
        out = [right[p, i] - search[p, i] for i in range(24)]
        total = None
        for i, v in enumerate(out):
            search[p, i] = v
            total = v * v if total is None else total + v * v
        sums[p] = total
        send_body(unflat(out, 4), 2, p, 1)
        return _

    beside = {
        0: [(first_send, 0, 6)],
        1: [(interior_guess, 0, 0)],
        2: [(second, 0, 2)],
        3: [(second, 2, 4)],
        4: [(second, 4, 6)],
        5: [(interior_field, 0, 0)],
        6: [(normal, 0, 2)],
        7: [(normal, 2, 4)],
        8: [(normal, 4, 6)],
    }
    for step in range(NSMEAR):
        items = smear_step(step, items, beside.get(step, []))
    items = list(items)
    start_right(items)
    finish_right(items, beside[NSMEAR])

    lax.fori_loop(0, PAIRS, third, 0)
    interior(search, 1)

    def fourth(p, _):
        out = receive_body(search, 2, p, 1)
        total = None
        for i, v in enumerate(out):
            field_b[p, i] = v
            total = v * v if total is None else total + v * v
        sums[PAIRS + p] = total
        send_body(unflat(out, 4), 3, p, -1)
        return _

    lax.fori_loop(0, PAIRS, fourth, 0)

    mine = jnp.zeros((8, 128), jnp.float32)
    for k in range(2 * PAIRS):
        mine = jnp.where(sh.lane == k, jnp.sum(sums[k], axis=1, keepdims=True), mine)
    slot = 0
    done_interior = False
    for stage, axis in enumerate(AXES):
        red_out[stage] = mine
        copies = []
        for k in range(1, n_of[axis]):
            copy = pltpu.make_async_remote_copy(
                src_ref=red_out.at[stage], dst_ref=red_in.at[slot],
                send_sem=r_send.at[slot], recv_sem=red_sem.at[slot],
                device_id=peer(axis, k), device_id_type=MESH,
            )
            copy.start()
            copies.append((copy, slot))
            slot += 1
        if not done_interior:
            interior(field_b, -1)
            done_interior = True
        for copy, place in copies:
            copy.wait()
            mine = mine + red_in[place]
    top = jnp.sum(mine[0:4], axis=0, keepdims=True)
    bottom = jnp.sum(mine[4:8], axis=0, keepdims=True)
    both = jnp.where(sh.low, top, bottom)
    curvature = pltpu.roll(both, 128 - PAIRS, 1)
    steps = both / jnp.where(sh.lane < PAIRS, curvature, 1.0)

    def last(p, _):
        out = receive_body(field_b, 3, p, -1)
        length = jnp.sum(jnp.where(sh.lane == p, steps, 0.0), axis=1, keepdims=True)
        first, second_rhs = rhs_of(p)
        for i, v in enumerate(out):
            s = search[p, i]
            res = s - length * v
            sol = guess[p, i] + length * s
            res_ref[first, i] = res[0:4]
            res_ref[second_rhs, i] = res[4:8]
            sol_ref[first, i] = sol[0:4]
            sol_ref[second_rhs, i] = sol[4:8]
        return _

    lax.fori_loop(0, PAIRS, last, 0)

    def drain(w, _):
        for p in range(0, PAIRS, EDGE_CHUNK):
            for d in range(4):
                edge_copy(w, d, p).wait_send()
        for p in range(0, PAIRS, TIME_CHUNK):
            for d in range(2):
                time_copy(w, d, p).wait_send()
        return _

    lax.fori_loop(0, 4, drain, 0)

    def drain_s(step, _):
        for d in range(4):
            sm_copy(step, d).wait_send()
        return _

    lax.fori_loop(0, NSMEAR + 1, drain_s, 0)
    for d in range(2):
        smt_copy(d).wait_send()


def on_device(sizes, links, guess, source_sites):
    rows, lanes = guess.shape[-2:]
    f32 = jnp.float32
    copies = sum(n - 1 for n in sizes)
    tile = (8, lanes)
    vm = lambda *shape: pltpu.VMEM(shape + tile, f32)
    dma = lambda *shape: pltpu.SemaphoreType.DMA(shape)
    out = jax.ShapeDtypeStruct((12, 24, rows, lanes), f32)
    sol, res = pl.pallas_call(
        functools.partial(kernel, sizes),
        out_shape=(out, out),
        in_specs=[
            pl.BlockSpec(memory_space=pltpu.SMEM),
            pl.BlockSpec(memory_space=pltpu.VMEM),
            pl.BlockSpec(memory_space=pltpu.VMEM),
        ],
        out_specs=(pl.BlockSpec(memory_space=pltpu.VMEM), pl.BlockSpec(memory_space=pltpu.VMEM)),
        scratch_shapes=[
            vm(72), vm(PAIRS, 24), vm(PAIRS, 24), vm(PAIRS, 24), vm(PAIRS, 24), vm(PAIRS, 24),
            vm(PAIRS, 24), vm(2, PAIRS, 12),
            vm(4, 4, PAIRS, 3), vm(4, 4, PAIRS, 3), vm(4, 2, PAIRS, 12), vm(4, 2, PAIRS, 12),
            vm(NSMEAR + 1, 4, 3), vm(NSMEAR + 1, 4, 3), vm(2, 12), vm(2, 12),
            vm(3), vm(copies), vm(2 * PAIRS),
            dma(4, 4, PAIRS), dma(4, 2, PAIRS), dma(4, 6, PAIRS),
            dma(NSMEAR + 1, 4), dma(2), dma(NSMEAR + 2, 4), dma(copies), dma(copies),
        ],
        compiler_params=pltpu.CompilerParams(
            collective_id=0, has_side_effects=True, vmem_limit_bytes=48 * 1024 * 1024
        ),
    )(
        source_sites.reshape(4),
        links.reshape(72, rows, lanes),
        guess.reshape(12, 24, rows, lanes),
    )
    return sol.reshape(guess.shape), res.reshape(guess.shape)


def solution(mesh):
    sizes = tuple(mesh.shape[axis] for axis in AXES)
    fields = P(None, None, None, None, "ta", "xy", "gz")
    return jax.shard_map(
        functools.partial(on_device, sizes),
        mesh=mesh,
        in_specs=(fields, fields, P("ta", "xy", "gz", None)),
        out_specs=(fields, fields),
        check_vma=False,
    )
```
